32 devices in a mesh: groups: 2 (over y), expert: 8 (over z, x), tensor: 2 (over core).
Axes of the slice: x: 2, y: 2, z: 4, core: 2. Of those that a mesh axis runs over, the one named last changes fastest.
Arguments:
- tokens: bfloat16 [1024, 1536], P(('groups', 'expert')), parts along dimension 0, may hold values from -12 to 12
- gain: float32 [1536], replicated, may hold values from 0.25 to 1.75
- route_ids: int32 [1024, 4], P(('groups', 'expert')), parts along dimension 0, may hold values from 0 to 3, as said below
- route_weights: float32 [1024, 4], P(('groups', 'expert')), parts along dimension 0, may hold values from 0.05 to 0.5
- w_gate: bfloat16 [8, 1536, 768], P('expert', None, 'tensor'), may hold values from -0.15625 to 0.15625
- w_up: bfloat16 [8, 1536, 768], P('expert', None, 'tensor'), may hold values from -0.15625 to 0.15625
- w_down: bfloat16 [8, 768, 1536], P('expert', 'tensor'), may hold values from -0.15625 to 0.15625
Outputs:
- mixed: bfloat16 [1024, 1536], P(('groups', 'expert')), parts along dimension 0
The draws below stay inside these ranges and needn't reach their ends.
There are 2 independent parts, one for each index of `groups`. The reference program is written for one: setup_inputs(seed, part) draws one part's arguments, and reference() takes and returns one part's arrays. A program takes and returns all parts, laid end to end along the dimension named above; an argument that names none is the same for every part. Nothing has to cross between parts.
Inputs may be any that keep to these rules, and one draw needn't show every extreme that they name: `route_ids`: each row names 4 different experts. In each aligned block of 32 rows no expert is named more than 32 times; one expert, the same in every block, is named exactly 32 times in every block, and the other experts' counts within a block differ by at most one.
All inputs are finite; a program needn't handle non-finite values.
Results may differ from the reference program's by a relative error of at most 0.0045.
Values may be sent and summed in bfloat16 or wider, within the bound.
A program may use at most 64 MiB of HBM per device.

```python
import math
import jax
import jax.numpy as jnp
from jax import lax

D = 1536
FF = 1536
TOP = 4
EXPERTS = 4
TOK_DEV = 32
CAP = 32
TOKENS = 512


def draw_tokens(key, part):
    key_base = jax.random.fold_in(key, 0)
    values = jax.random.normal(key_base, (TOKENS, D), jnp.float32)
    return jnp.clip(values, -12.0, 12.0).astype(jnp.bfloat16)


def draw_route_ids(key, part):
    blocks = TOKENS // TOK_DEV
    slot_total = TOK_DEV * TOP
    others = EXPERTS - 1
    key_hot, key_rank, key_rows, key_cols = jax.random.split(key, 4)
    hot_expert = jax.random.randint(key_hot, (), 0, EXPERTS, dtype=jnp.int32)
    spare = slot_total - CAP
    floor_count = spare // others
    surplus = spare - floor_count * others
    rank_keys = jax.random.split(key_rank, blocks)
    ranking = jax.vmap(lambda sub_key: jax.random.permutation(sub_key, others))(rank_keys)
    counts = floor_count + (ranking < surplus).astype(jnp.int32)
    run_ends = CAP + jnp.cumsum(counts, axis=1, dtype=jnp.int32)
    places = jnp.arange(slot_total, dtype=jnp.int32)
    owner_index = jnp.sum((places[None, :, None] >= run_ends[:, None, :]).astype(jnp.int32), axis=2, dtype=jnp.int32)
    other_ids = (hot_expert + 1 + owner_index) % EXPERTS
    listed = jnp.where(places[None, :] < CAP, hot_expert, other_ids)
    id_grid = listed.reshape(blocks, TOP, TOK_DEV).transpose(0, 2, 1)
    row_keys = jax.random.split(key_rows, blocks)
    row_order = jax.vmap(lambda sub_key: jax.random.permutation(sub_key, TOK_DEV))(row_keys)
    id_grid = jnp.take_along_axis(id_grid, row_order[:, :, None], axis=1)
    scores = jax.random.randint(key_cols, (blocks, TOK_DEV, TOP), 0, 1 << 20, dtype=jnp.int32) * TOP + jnp.arange(TOP, dtype=jnp.int32)
    col_order = jnp.argsort(scores, axis=2)
    id_grid = jnp.take_along_axis(id_grid, col_order, axis=2)
    return id_grid.reshape(TOKENS, TOP).astype(jnp.int32)


def steps_of(own_key, dims, pieces, least, top_value):
    factor_of = 1.0
    for axis_at, parts in pieces:
        draws = jax.random.uniform(jax.random.fold_in(jax.random.fold_in(own_key, 6), axis_at), (parts,), jnp.float32, least / len(pieces), top_value / len(pieces))
        factor_of = factor_of * jnp.repeat(jnp.exp(draws), dims[axis_at] // parts).reshape((-1,) + (1,) * (len(dims) - 1 - axis_at))
    return factor_of


def normal_values(key, extent, deviation, limit, shards=(), held_as=jnp.bfloat16):
    level = steps_of(key, extent, shards, -0.22, 0.18) if shards else 1.0
    entries = jax.random.normal(key, extent, jnp.float32) * deviation * level
    return jnp.minimum(jnp.maximum(entries, -limit), limit).astype(held_as)


def setup_inputs(seed: int = 0, part: int = 0) -> dict:
    arg_keys = jax.random.split(jax.random.key(seed), 8)
    part_splits = jax.random.split(jax.random.fold_in(arg_keys[7], part), 8)
    tokens = draw_tokens(jax.random.fold_in(jax.random.fold_in(arg_keys[7], part), 71), part)
    gain = jnp.clip(1.0 + 0.15 * jax.random.normal(arg_keys[1], (D,), jnp.float32), 0.25, 1.75)
    route_ids = draw_route_ids(jax.random.fold_in(jax.random.fold_in(arg_keys[7], part), 71), part)
    route_weights = jnp.clip(jnp.exp(math.log(0.5) - 2.3025851 * jax.random.uniform(part_splits[3], (TOKENS, TOP), jnp.float32) ** steps_of(part_splits[3], (TOKENS, TOP), ((0, 8),), -0.2, 0.2)), 0.05, 0.5)
    w_gate = normal_values(arg_keys[4], (2 * EXPERTS, D, FF // 2), D ** -0.5, 0.15625, ((0, 8), (2, 2)))
    w_up = normal_values(arg_keys[5], (2 * EXPERTS, D, FF // 2), D ** -0.5, 0.15625, ((0, 8), (2, 2)))
    w_down = normal_values(arg_keys[6], (2 * EXPERTS, FF // 2, D), FF ** -0.5, 0.15625, ((0, 8), (1, 2)))
    return {"tokens": tokens, "gain": gain, "route_ids": route_ids, "route_weights": route_weights, "w_gate": w_gate, "w_up": w_up, "w_down": w_down}


def gated_unit(gate_val, up_val):
    return gate_val * jax.nn.sigmoid(1.702 * gate_val) * (up_val + 1.0)

def reference(tokens, gain, route_ids, route_weights, w_gate, w_up, w_down):
    resident = tokens.astype(jnp.float32)
    inv_rms = lax.rsqrt(lax.optimization_barrier(jnp.mean(resident * resident, axis=1, keepdims=True)) + 1e-05)
    normed = (resident * inv_rms * gain).astype(jnp.bfloat16)
    flat_ids = route_ids.reshape(-1)
    flat_weight = route_weights.reshape(-1)
    slot_total = flat_ids.shape[0]
    most_rows = TOKENS // TOK_DEV * CAP
    slot_range = jnp.arange(slot_total, dtype=jnp.int32)
    row_range = jnp.arange(most_rows, dtype=jnp.int32)

    def one_expert(summed, expert):
        chosen = flat_ids == expert
        rank_in = jnp.cumsum(chosen.astype(jnp.int32), dtype=jnp.int32) - 1
        target = jnp.where(chosen, rank_in, most_rows).astype(jnp.int32)
        picked = jnp.zeros((most_rows,), jnp.int32).at[target].set(slot_range, mode='drop')
        is_live = row_range < jnp.sum(chosen.astype(jnp.int32), dtype=jnp.int32)
        token_row = picked // TOP
        inputs = normed[token_row]
        first = (2 * expert).astype(jnp.int32)
        pair_gate = lax.dynamic_slice_in_dim(w_gate, first, 2, 0)
        pair_up = lax.dynamic_slice_in_dim(w_up, first, 2, 0)
        pair_down = lax.dynamic_slice_in_dim(w_down, first, 2, 0)
        full_gate = jnp.concatenate([pair_gate[0], pair_gate[1]], axis=1)
        full_up = jnp.concatenate([pair_up[0], pair_up[1]], axis=1)
        full_down = pair_down.reshape(-1, pair_down.shape[2])
        gate_val = jnp.dot(inputs, full_gate, preferred_element_type=jnp.float32)
        up_val = jnp.dot(inputs, full_up, preferred_element_type=jnp.float32)
        hidden = gated_unit(gate_val, up_val).astype(jnp.bfloat16)
        expert_out = jnp.dot(hidden, full_down, preferred_element_type=jnp.float32)
        weight = jnp.where(is_live, flat_weight[picked], 0.0)
        summed = summed.at[token_row].add(weight[:, None] * expert_out)
        return (summed, None)
    empty_sum = jnp.zeros(resident.shape, jnp.float32)
    summed, unused = lax.scan(one_expert, empty_sum, jnp.arange(EXPERTS, dtype=jnp.int32))
    return (resident + summed).astype(jnp.bfloat16)
```

```python
import functools

import jax
import jax.numpy as jnp
from jax import lax
from jax.experimental import pallas as pl
from jax.experimental.pallas import tpu as pltpu
from jax.sharding import PartitionSpec as P

MESH = pl.DeviceIdType.MESH


def gated_unit(gate_val, up_val):
    return gate_val * jax.nn.sigmoid(1.702 * gate_val) * (up_val + 1.0)


def flipped(index, bits, count):
    out = index
    power = 1
    while power < count:
        if bits // power % 2:
            out = out + power - 2 * power * lax.rem(index // power, 2)
        power *= 2
    return out


def dense_kernel(
    experts,
    tokens_ref,
    gain_ref,
    ids_ref,
    weights_ref,
    gate_ref,
    up_ref,
    down_ref,
    out_ref,
    wg,
    wu,
    wd,
    xa,
    xb,
    own_out,
    x_send,
    x_recv,
    z_send,
    z_recv,
    final,
    load_sem,
    swap_send,
    swap_recv,
    xa_send,
    xa_recv,
    xb_send,
    xb_recv,
    px_send,
    px_recv,
    pz_send,
    pz_recv,
    last_send,
    last_recv,
):
    me = lax.axis_index("expert")
    core = lax.axis_index("tensor")
    place = me // 2
    side = lax.rem(me, 2)
    across = {"expert": place * 2 + 1 - side}
    sibling = {"tensor": 1 - core}
    along = [{"expert": flipped(place, k, experts) * 2 + side} for k in range(experts)]
    rows = xa.shape[1]
    cols = gate_ref.shape[2]

    barrier = pltpu.get_barrier_semaphore()
    for peer in [across, sibling] + along[1:]:
        pl.semaphore_signal(barrier, inc=1, device_id=peer, device_id_type=MESH)

    pairs = (
        (gate_ref.at[0], lambda half: wg.at[:, pl.ds(half * cols, cols)]),
        (up_ref.at[0], lambda half: wu.at[:, pl.ds(half * cols, cols)]),
        (down_ref.at[0], lambda half: wd.at[pl.ds(half * cols, cols), :]),
    )
    loads = [
        pltpu.make_async_copy(src, dst(0), load_sem.at[i]) for i, (src, dst) in enumerate(pairs)
    ]
    for load in loads:
        load.start()

    first = pl.multiple_of(core * rows, rows)
    own = pl.ds(first, rows)
    resident = tokens_ref[own, :].astype(jnp.float32)
    inv_rms = lax.rsqrt(jnp.mean(resident * resident, axis=1, keepdims=True) + 1e-05)
    xa[0] = (resident * inv_rms * gain_ref[...]).astype(jnp.bfloat16)

    pl.semaphore_wait(barrier, experts + 1)

    def remote(src, dst, send, recv, peer):
        return pltpu.make_async_remote_copy(
            src_ref=src, dst_ref=dst, send_sem=send, recv_sem=recv, device_id=peer,
            device_id_type=MESH,
        )

    gather_z = [
        remote(xa.at[0], xa.at[k], xa_send.at[k], xa_recv.at[k], along[k]) if k else None
        for k in range(experts)
    ]
    gather_x = [
        remote(xa.at[k], xb.at[k], xb_send.at[k], xb_recv.at[k], across) for k in range(experts)
    ]
    part_x = [
        remote(x_send.at[k], x_recv.at[k], px_send.at[k], px_recv.at[k], across)
        for k in range(experts)
    ]
    part_z = [
        remote(z_send.at[k], z_recv.at[k], pz_send.at[k], pz_recv.at[k], along[k]) if k else None
        for k in range(experts)
    ]
    swaps = [
        remote(src, dst(1), swap_send.at[i], swap_recv.at[i], sibling)
        for i, (src, dst) in enumerate(pairs)
    ]

    gather_x[0].start()
    for k in range(1, experts):
        gather_z[k].start()
    for swap in swaps:
        swap.start()

    def close(k):
        part_x[k].wait_recv()
        both = own_out[k] + x_recv[k].astype(jnp.float32)
        if k:
            z_send[k] = both.astype(jnp.bfloat16)
            part_z[k].start()
        else:
            own_out[0] = both

    for k in range(experts):
        if k + 1 < experts:
            gather_z[k + 1].wait_recv()
            gather_x[k + 1].start()
        gather_x[k].wait_recv()
        block = jnp.concatenate([xb[k], xa[k]], axis=0)
        if k == 0:
            loads[0].wait()
            swaps[0].wait_recv()
        gate_val = jnp.dot(block, wg[...], preferred_element_type=jnp.float32)
        if k == 0:
            loads[1].wait()
            swaps[1].wait_recv()
        up_val = jnp.dot(block, wu[...], preferred_element_type=jnp.float32)
        hidden = gated_unit(gate_val, up_val).astype(jnp.bfloat16)
        if k == 0:
            loads[2].wait()
            swaps[2].wait_recv()
        result = jnp.dot(hidden, wd[...], preferred_element_type=jnp.float32)
        x_send[k] = result[:rows].astype(jnp.bfloat16)
        part_x[k].start()
        own_out[k] = result[rows:]
        if k:
            close(k - 1)
    close(experts - 1)

    ids = ids_ref[own, :]
    shares = weights_ref[own, :]
    total = tokens_ref[own, :].astype(jnp.float32)
    for k in range(experts):
        expert = flipped(place, k, experts)
        share = jnp.sum(jnp.where(ids == expert, shares, 0.0), axis=1, keepdims=True)
        if k:
            part_z[k].wait_recv()
            value = z_recv[k].astype(jnp.float32)
        else:
            value = own_out[0]
        total = total + share * value
    final[...] = total.astype(jnp.bfloat16)
    last = remote(final, out_ref.at[own, :], last_send, last_recv, sibling)
    last.start()
    out_ref[own, :] = final[...]

    for k in range(experts):
        gather_x[k].wait_send()
        part_x[k].wait_send()
        if k:
            gather_z[k].wait_send()
            part_z[k].wait_send()
    for swap in swaps:
        swap.wait_send()
    last.wait_send()
    last.wait_recv()


def dense_layer(tokens, gain, route_ids, route_weights, w_gate, w_up, w_down):
    experts = lax.axis_size("expert") // 2
    features = tokens.shape[1]
    rows = tokens.shape[0] // lax.axis_size("tensor")
    units = 2 * w_gate.shape[2]
    vmem = pl.BlockSpec(memory_space=pltpu.VMEM)
    hbm = pl.BlockSpec(memory_space=pltpu.HBM)
    half = jnp.bfloat16
    dma = pltpu.SemaphoreType.DMA
    slots = pltpu.VMEM((experts, rows, features), half)
    return pl.pallas_call(
        functools.partial(dense_kernel, experts),
        out_shape=jax.ShapeDtypeStruct(tokens.shape, tokens.dtype),
        in_specs=[vmem] * 4 + [hbm] * 3,
        out_specs=vmem,
        scratch_shapes=[
            pltpu.VMEM((features, units), half),
            pltpu.VMEM((features, units), half),
            pltpu.VMEM((units, features), half),
            slots,
            slots,
            pltpu.VMEM((experts, rows, features), jnp.float32),
            slots,
            slots,
            slots,
            slots,
            pltpu.VMEM((rows, features), half),
            dma((3,)),
            dma((3,)),
            dma((3,)),
        ]
        + [dma((experts,))] * 8
        + [dma, dma],
        compiler_params=pltpu.CompilerParams(
            collective_id=0, has_side_effects=True, vmem_limit_bytes=48 * 1024 * 1024
        ),
    )(tokens, gain.reshape(1, features), route_ids, route_weights, w_gate, w_up, w_down)


def route_tables(chosen_ids, chosen_weights, expert_count, slot_room):
    row_count, top_count = chosen_ids.shape
    matches = (chosen_ids[:, :, None] == jnp.arange(expert_count, dtype=jnp.int32)).astype(
        jnp.float32
    )
    flat_match = matches.reshape(row_count * top_count, expert_count)
    order_range = jnp.arange(row_count * top_count, dtype=jnp.int32)
    earlier = (order_range[:, None] > order_range[None, :]).astype(jnp.float32)
    before = jnp.dot(
        earlier, flat_match, precision=lax.Precision.HIGHEST, preferred_element_type=jnp.float32
    )
    position = jnp.sum(before * flat_match, axis=1).reshape(row_count, top_count).astype(jnp.int32)
    slot_index = chosen_ids * slot_room + position
    targets = jnp.arange(expert_count * slot_room, dtype=jnp.int32)
    slot_hits = slot_index[None, :, :] == targets[:, None, None]
    send_table = jnp.sum(slot_hits.astype(jnp.float32), axis=2).astype(jnp.bfloat16)
    mix_table = jnp.sum(jnp.where(slot_hits, chosen_weights[None, :, :], 0.0), axis=2)
    return (send_table, mix_table)


def routed_layer(tokens, gain, route_ids, route_weights, w_gate, w_up, w_down):
    expert_axis = lax.axis_size("expert")
    expert_count = expert_axis // 2
    tensor_count = lax.axis_size("tensor")
    own_rows = tokens.shape[0] // tensor_count
    top_count = route_ids.shape[1]
    capacity = max(2, own_rows * top_count // expert_count)
    gate_local = w_gate[0]
    up_local = w_up[0]
    down_local = w_down[0]
    first_row = lax.axis_index("tensor") * own_rows
    own_tokens = lax.dynamic_slice_in_dim(tokens, first_row, own_rows, 0)
    own_ids = lax.dynamic_slice_in_dim(route_ids, first_row, own_rows, 0)
    own_weights = lax.dynamic_slice_in_dim(route_weights, first_row, own_rows, 0)
    resident = own_tokens.astype(jnp.float32)
    inv_rms = lax.rsqrt(jnp.mean(resident * resident, axis=1, keepdims=True) + 1e-05)
    normed = (resident * inv_rms * gain).astype(jnp.bfloat16)
    send_table, mix_table = route_tables(own_ids, own_weights, expert_count, capacity)
    packed = jnp.dot(send_table, normed, preferred_element_type=jnp.float32).astype(jnp.bfloat16)
    features = packed.shape[1]
    by_expert = packed.reshape(expert_count, 1, capacity, features)
    outgoing = jnp.broadcast_to(by_expert, (expert_count, 2, capacity, features)).reshape(
        expert_axis * capacity, features
    )
    arrived = lax.all_to_all(outgoing, "expert", split_axis=0, concat_axis=0, tiled=True)
    row_piece = lax.all_gather(arrived, "tensor", axis=0, tiled=True)
    gate_val = jnp.dot(row_piece, gate_local, preferred_element_type=jnp.float32)
    up_val = jnp.dot(row_piece, up_local, preferred_element_type=jnp.float32)
    hidden = gated_unit(gate_val, up_val).astype(jnp.bfloat16)
    partial_value = lax.psum_scatter(
        jnp.dot(hidden, down_local, preferred_element_type=jnp.float32),
        "tensor",
        scatter_dimension=0,
        tiled=True,
    )
    returned = lax.all_to_all(
        partial_value.astype(jnp.bfloat16), "expert", split_axis=0, concat_axis=0, tiled=True
    ).astype(partial_value.dtype)
    expert_out = (
        returned.reshape(expert_count, 2, capacity, features)
        .sum(axis=1)
        .reshape(expert_count * capacity, features)
    )
    weighted = jnp.dot(
        mix_table.T, expert_out, precision=lax.Precision.HIGHEST, preferred_element_type=jnp.float32
    )
    finished = (resident + weighted).astype(jnp.bfloat16)
    return lax.all_gather(finished, "tensor", axis=0, tiled=True)


def per_device(tokens, gain, route_ids, route_weights, w_gate, w_up, w_down):
    experts = lax.axis_size("expert") // 2
    dense = (
        route_ids.shape[1] == experts
        and experts & (experts - 1) == 0
        and lax.axis_size("tensor") == 2
        and w_gate.shape[0] == 1
    )
    layer = dense_layer if dense else routed_layer
    return layer(tokens, gain, route_ids, route_weights, w_gate, w_up, w_down)


def solution(mesh):
    placed = (
        P(("groups", "expert"), None),
        P(),
        P(("groups", "expert"), None),
        P(("groups", "expert"), None),
        P("expert", None, "tensor"),
        P("expert", None, "tensor"),
        P("expert", "tensor", None),
    )
    return jax.shard_map(
        per_device,
        mesh=mesh,
        in_specs=placed,
        out_specs=P(("groups", "expert"), None),
        check_vma=False,
    )
```

```python
import functools

import jax
import jax.numpy as jnp
from jax import lax
from jax.experimental import pallas as pl
from jax.experimental.pallas import tpu as pltpu
from jax.sharding import PartitionSpec as P

MESH = pl.DeviceIdType.MESH


def gated_unit(gate_val, up_val):
    return gate_val * jax.nn.sigmoid(1.702 * gate_val) * (up_val + 1.0)


def flipped(index, bits, count):
    out = index
    power = 1
    while power < count:
        if bits // power % 2:
            out = out + power - 2 * power * lax.rem(index // power, 2)
        power *= 2
    return out


def dense_kernel(
    experts,
    tokens_ref,
    gain_ref,
    ids_ref,
    weights_ref,
    gate_ref,
    up_ref,
    down_ref,
    out_ref,
    held,
    gain,
    ids,
    weights,
    wg,
    wu,
    wd,
    xa,
    xb,
    own_out,
    x_send,
    x_recv,
    z_send,
    z_recv,
    final,
    small_sem,
    load_sem,
    swap_send,
    swap_recv,
    xa_send,
    xa_recv,
    xb_send,
    xb_recv,
    px_send,
    px_recv,
    pz_send,
    pz_recv,
    last_send,
    last_recv,
):
    me = lax.axis_index("expert")
    core = lax.axis_index("tensor")
    place = me // 2
    side = lax.rem(me, 2)
    across = {"expert": place * 2 + 1 - side}
    sibling = {"tensor": 1 - core}
    along = [{"expert": flipped(place, k, experts) * 2 + side} for k in range(experts)]
    pieces, rows, width = xa.shape[1:]
    cols = gate_ref.shape[2]
    own = pl.ds(pl.multiple_of(core * rows, rows), rows)

    barrier = pltpu.get_barrier_semaphore()
    for peer in [across, sibling] + along[1:]:
        pl.semaphore_signal(barrier, inc=1, device_id=peer, device_id_type=MESH)

    smalls = [
        pltpu.make_async_copy(src, dst, small_sem.at[i])
        for i, (src, dst) in enumerate(
            (
                (tokens_ref.at[own, :], held),
                (gain_ref, gain),
                (ids_ref, ids),
                (weights_ref, weights),
            )
        )
    ]
    for small in smalls:
        small.start()

    pairs = (
        (gate_ref.at[0], lambda half: wg.at[:, pl.ds(half * cols, cols)]),
        (up_ref.at[0], lambda half: wu.at[:, pl.ds(half * cols, cols)]),
        (down_ref.at[0], lambda half: wd.at[pl.ds(half * cols, cols), :]),
    )
    loads = [
        pltpu.make_async_copy(src, dst(0), load_sem.at[i]) for i, (src, dst) in enumerate(pairs)
    ]
    for load in loads:
        load.start()

    def part(p):
        return pl.ds(p * width, width)

    smalls[0].wait()
    resident = held[...].astype(jnp.float32)
    inv_rms = lax.rsqrt(jnp.mean(resident * resident, axis=1, keepdims=True) + 1e-05)
    smalls[1].wait()
    normed = (resident * inv_rms * gain[...].reshape(1, -1)).astype(jnp.bfloat16)
    for p in range(pieces):
        xa[0, p] = normed[:, p * width : (p + 1) * width]

    pl.semaphore_wait(barrier, experts + 1)

    def remote(src, dst, send, recv, peer):
        return pltpu.make_async_remote_copy(
            src_ref=src, dst_ref=dst, send_sem=send, recv_sem=recv, device_id=peer,
            device_id_type=MESH,
        )

    def gather_z(k, p):
        return remote(xa.at[0, p], xa.at[k, p], xa_send.at[k, p], xa_recv.at[k, p], along[k])

    def gather_x(k, p):
        return remote(xa.at[k, p], xb.at[k, p], xb_send.at[k, p], xb_recv.at[k, p], across)

    def part_x(k, p):
        return remote(
            x_send.at[k, p], x_recv.at[k, p], px_send.at[k, p], px_recv.at[k, p], across
        )

    def part_z(k, p):
        return remote(
            z_send.at[k, p], z_recv.at[k, p], pz_send.at[k, p], pz_recv.at[k, p], along[k]
        )

    swaps = [
        remote(src, dst(1), swap_send.at[i], swap_recv.at[i], sibling)
        for i, (src, dst) in enumerate(pairs)
    ]

    for p in range(pieces):
        gather_x(0, p).start()
        if experts > 1:
            gather_z(1, p).start()
    for k in range(2, experts):
        for p in range(pieces):
            gather_z(k, p).start()
    for swap in swaps:
        swap.start()

    smalls[2].wait()
    smalls[3].wait()
    tokens_here = ids.shape[1]
    row_at = lax.broadcasted_iota(jnp.int32, (rows, tokens_here), 0) + core * rows
    on_row = row_at == lax.broadcasted_iota(jnp.int32, (rows, tokens_here), 1)
    shares = []
    for k in range(experts):
        named = jnp.where(ids[...] == flipped(place, k, experts), weights[...], 0.0)
        line = jnp.sum(named, axis=0, keepdims=True)
        shares.append(jnp.sum(jnp.where(on_row, line, 0.0), axis=1, keepdims=True))

    def forward(k):
        for p in range(pieces):
            gather_z(k, p).wait_recv()
            gather_x(k, p).start()

    def product(k, table):
        value = None
        for p in range(pieces):
            block = jnp.concatenate([xb[k, p], xa[k, p]], axis=0)
            term = jnp.dot(block, table[part(p), :], preferred_element_type=jnp.float32)
            value = term if value is None else value + term
        return value

    def compute(k):
        for p in range(pieces):
            gather_x(k, p).wait_recv()
        if k == 0:
            loads[0].wait()
            swaps[0].wait_recv()
        gate_val = product(k, wg)
        if k == 0:
            loads[1].wait()
            swaps[1].wait_recv()
        up_val = product(k, wu)
        hidden = gated_unit(gate_val, up_val).astype(jnp.bfloat16)
        if k == 0:
            loads[2].wait()
            swaps[2].wait_recv()
        for p in range(pieces):
            result = jnp.dot(hidden, wd[:, part(p)], preferred_element_type=jnp.float32)
            x_send[k, p] = result[:rows].astype(jnp.bfloat16)
            if k:
                part_x(k, p).start()
            own_out[k, p] = result[rows:]

    def close(k):
        for p in range(pieces):
            part_x(k, p).wait_recv()
            both = own_out[k, p] + x_recv[k, p].astype(jnp.float32)
            z_send[k, p] = both.astype(jnp.bfloat16)
            part_z(k, p).start()

    for k in range(experts):
        if k + 1 < experts:
            forward(k + 1)
        if k >= 3:
            close(k - 2)
        compute(k)
    for p in range(pieces):
        part_x(0, p).start()
    for k in range(max(1, experts - 2), experts):
        close(k)

    for p in range(pieces):
        part_x(0, p).wait_recv()
        both = own_out[0, p] + x_recv[0, p].astype(jnp.float32)
        own_out[0, p] = held[:, part(p)].astype(jnp.float32) + shares[0] * both
    for p in range(pieces):
        total = own_out[0, p]
        for k in range(1, experts):
            part_z(k, p).wait_recv()
            total = total + shares[k] * z_recv[k, p].astype(jnp.float32)
        final[:, part(p)] = total.astype(jnp.bfloat16)
        remote(
            final.at[:, part(p)], out_ref.at[own, part(p)], last_send.at[p], last_recv.at[p],
            sibling,
        ).start()
        out_ref[own, part(p)] = total.astype(jnp.bfloat16)

    for p in range(pieces):
        for k in range(experts):
            gather_x(k, p).wait_send()
            part_x(k, p).wait_send()
            if k:
                gather_z(k, p).wait_send()
                part_z(k, p).wait_send()
    for swap in swaps:
        swap.wait_send()
    for p in range(pieces):
        remote(
            final.at[:, part(p)], out_ref.at[own, part(p)], last_send.at[p], last_recv.at[p],
            sibling,
        ).wait()


def dense_layer(tokens, gain, route_ids, route_weights, w_gate, w_up, w_down):
    experts = lax.axis_size("expert") // 2
    features = tokens.shape[1]
    rows = tokens.shape[0] // lax.axis_size("tensor")
    units = 2 * w_gate.shape[2]
    pieces = 2
    vmem = pl.BlockSpec(memory_space=pltpu.VMEM)
    hbm = pl.BlockSpec(memory_space=pl.ANY)
    half = jnp.bfloat16
    dma = pltpu.SemaphoreType.DMA
    slots = pltpu.VMEM((experts, pieces, rows, features // pieces), half)
    ids = route_ids.T
    weights = route_weights.T
    return pl.pallas_call(
        functools.partial(dense_kernel, experts),
        out_shape=jax.ShapeDtypeStruct(tokens.shape, tokens.dtype),
        in_specs=[hbm] * 7,
        out_specs=vmem,
        scratch_shapes=[
            pltpu.VMEM((rows, features), half),
            pltpu.VMEM((features,), jnp.float32),
            pltpu.VMEM(ids.shape, jnp.int32),
            pltpu.VMEM(weights.shape, jnp.float32),
            pltpu.VMEM((features, units), half),
            pltpu.VMEM((features, units), half),
            pltpu.VMEM((units, features), half),
            slots,
            slots,
            pltpu.VMEM((experts, pieces, rows, features // pieces), jnp.float32),
            slots,
            slots,
            slots,
            slots,
            pltpu.VMEM((rows, features), half),
            dma((4,)),
            dma((3,)),
            dma((3,)),
            dma((3,)),
        ]
        + [dma((experts, pieces))] * 8
        + [dma((pieces,))] * 2,
        compiler_params=pltpu.CompilerParams(
            collective_id=0, has_side_effects=True, vmem_limit_bytes=66_000_000
        ),
    )(tokens, gain, ids, weights, w_gate, w_up, w_down)


def route_tables(chosen_ids, chosen_weights, expert_count, slot_room):
    row_count, top_count = chosen_ids.shape
    matches = (chosen_ids[:, :, None] == jnp.arange(expert_count, dtype=jnp.int32)).astype(
        jnp.float32
    )
    flat_match = matches.reshape(row_count * top_count, expert_count)
    order_range = jnp.arange(row_count * top_count, dtype=jnp.int32)
    earlier = (order_range[:, None] > order_range[None, :]).astype(jnp.float32)
    before = jnp.dot(
        earlier, flat_match, precision=lax.Precision.HIGHEST, preferred_element_type=jnp.float32
    )
    position = jnp.sum(before * flat_match, axis=1).reshape(row_count, top_count).astype(jnp.int32)
    slot_index = chosen_ids * slot_room + position
    targets = jnp.arange(expert_count * slot_room, dtype=jnp.int32)
    slot_hits = slot_index[None, :, :] == targets[:, None, None]
    send_table = jnp.sum(slot_hits.astype(jnp.float32), axis=2).astype(jnp.bfloat16)
    mix_table = jnp.sum(jnp.where(slot_hits, chosen_weights[None, :, :], 0.0), axis=2)
    return (send_table, mix_table)


def routed_layer(tokens, gain, route_ids, route_weights, w_gate, w_up, w_down):
    expert_axis = lax.axis_size("expert")
    expert_count = expert_axis // 2
    tensor_count = lax.axis_size("tensor")
    own_rows = tokens.shape[0] // tensor_count
    top_count = route_ids.shape[1]
    capacity = max(2, own_rows * top_count // expert_count)
    gate_local = w_gate[0]
    up_local = w_up[0]
    down_local = w_down[0]
    first_row = lax.axis_index("tensor") * own_rows
    own_tokens = lax.dynamic_slice_in_dim(tokens, first_row, own_rows, 0)
    own_ids = lax.dynamic_slice_in_dim(route_ids, first_row, own_rows, 0)
    own_weights = lax.dynamic_slice_in_dim(route_weights, first_row, own_rows, 0)
    resident = own_tokens.astype(jnp.float32)
    inv_rms = lax.rsqrt(jnp.mean(resident * resident, axis=1, keepdims=True) + 1e-05)
    normed = (resident * inv_rms * gain).astype(jnp.bfloat16)
    send_table, mix_table = route_tables(own_ids, own_weights, expert_count, capacity)
    packed = jnp.dot(send_table, normed, preferred_element_type=jnp.float32).astype(jnp.bfloat16)
    features = packed.shape[1]
    by_expert = packed.reshape(expert_count, 1, capacity, features)
    outgoing = jnp.broadcast_to(by_expert, (expert_count, 2, capacity, features)).reshape(
        expert_axis * capacity, features
    )
    arrived = lax.all_to_all(outgoing, "expert", split_axis=0, concat_axis=0, tiled=True)
    row_piece = lax.all_gather(arrived, "tensor", axis=0, tiled=True)
    gate_val = jnp.dot(row_piece, gate_local, preferred_element_type=jnp.float32)
    up_val = jnp.dot(row_piece, up_local, preferred_element_type=jnp.float32)
    hidden = gated_unit(gate_val, up_val).astype(jnp.bfloat16)
    partial_value = lax.psum_scatter(
        jnp.dot(hidden, down_local, preferred_element_type=jnp.float32),
        "tensor",
        scatter_dimension=0,
        tiled=True,
    )
    returned = lax.all_to_all(
        partial_value.astype(jnp.bfloat16), "expert", split_axis=0, concat_axis=0, tiled=True
    ).astype(partial_value.dtype)
    expert_out = (
        returned.reshape(expert_count, 2, capacity, features)
        .sum(axis=1)
        .reshape(expert_count * capacity, features)
    )
    weighted = jnp.dot(
        mix_table.T, expert_out, precision=lax.Precision.HIGHEST, preferred_element_type=jnp.float32
    )
    finished = (resident + weighted).astype(jnp.bfloat16)
    return lax.all_gather(finished, "tensor", axis=0, tiled=True)


def per_device(tokens, gain, route_ids, route_weights, w_gate, w_up, w_down):
    experts = lax.axis_size("expert") // 2
    dense = (
        route_ids.shape[1] == experts
        and experts & (experts - 1) == 0
        and lax.axis_size("tensor") == 2
        and w_gate.shape[0] == 1
    )
    layer = dense_layer if dense else routed_layer
    return layer(tokens, gain, route_ids, route_weights, w_gate, w_up, w_down)


def solution(mesh):
    placed = (
        P(("groups", "expert"), None),
        P(),
        P(("groups", "expert"), None),
        P(("groups", "expert"), None),
        P("expert", None, "tensor"),
        P("expert", None, "tensor"),
        P("expert", "tensor", None),
    )
    return jax.shard_map(
        per_device,
        mesh=mesh,
        in_specs=placed,
        out_specs=P(("groups", "expert"), None),
        check_vma=False,
    )
```

```python
import functools

import jax
import jax.numpy as jnp
from jax import lax
from jax.experimental import pallas as pl
from jax.experimental.pallas import tpu as pltpu
from jax.sharding import PartitionSpec as P

MESH = pl.DeviceIdType.MESH


def gated_unit(gate_val, up_val):
    return gate_val * jax.nn.sigmoid(1.702 * gate_val) * (up_val + 1.0)


def flipped(index, bits, count):
    out = index
    power = 1
    while power < count:
        if bits // power % 2:
            out = out + power - 2 * power * lax.rem(index // power, 2)
        power *= 2
    return out


def dense_kernel(
    experts,
    tokens_ref,
    gain_ref,
    ids_ref,
    weights_ref,
    gate_ref,
    up_ref,
    down_ref,
    out_ref,
    held,
    gain,
    ids,
    weights,
    wg,
    wu,
    wd,
    xa,
    xb,
    own_out,
    x_send,
    x_recv,
    z_send,
    z_recv,
    final,
    small_sem,
    load_sem,
    swap_send,
    swap_recv,
    xa_send,
    xa_recv,
    xb_send,
    xb_recv,
    px_send,
    px_recv,
    pz_send,
    pz_recv,
    last_send,
    last_recv,
    keep_sem,
):
    me = lax.axis_index("expert")
    core = lax.axis_index("tensor")
    place = me // 2
    side = lax.rem(me, 2)
    across = {"expert": place * 2 + 1 - side}
    sibling = {"tensor": 1 - core}
    along = [{"expert": flipped(place, k, experts) * 2 + side} for k in range(experts)]
    pieces, rows, width = xa.shape[1:]
    cols = gate_ref.shape[2]
    own = pl.ds(pl.multiple_of(core * rows, rows), rows)

    barrier = pltpu.get_barrier_semaphore()
    for peer in [across, sibling] + along[1:]:
        pl.semaphore_signal(barrier, inc=1, device_id=peer, device_id_type=MESH)

    smalls = [
        pltpu.make_async_copy(src, dst, small_sem.at[i])
        for i, (src, dst) in enumerate(
            (
                (tokens_ref.at[own, :], held),
                (gain_ref, gain),
                (ids_ref, ids),
                (weights_ref, weights),
            )
        )
    ]
    for small in smalls:
        small.start()

    pairs = (
        (gate_ref.at[0], lambda half: wg.at[:, pl.ds(half * cols, cols)]),
        (up_ref.at[0], lambda half: wu.at[:, pl.ds(half * cols, cols)]),
        (down_ref.at[0], lambda half: wd.at[pl.ds(half * cols, cols), :]),
    )
    loads = [
        pltpu.make_async_copy(src, dst(0), load_sem.at[i]) for i, (src, dst) in enumerate(pairs)
    ]
    for load in loads:
        load.start()

    def part(p):
        return pl.ds(p * width, width)

    smalls[0].wait()
    resident = held[...].astype(jnp.float32)
    inv_rms = lax.rsqrt(jnp.mean(resident * resident, axis=1, keepdims=True) + 1e-05)
    smalls[1].wait()
    normed = (resident * inv_rms * gain[...].reshape(1, -1)).astype(jnp.bfloat16)
    for p in range(pieces):
        xa[0, p] = normed[:, p * width : (p + 1) * width]

    pl.semaphore_wait(barrier, experts + 1)

    def remote(src, dst, send, recv, peer):
        return pltpu.make_async_remote_copy(
            src_ref=src, dst_ref=dst, send_sem=send, recv_sem=recv, device_id=peer,
            device_id_type=MESH,
        )

    def gather_z(k, p):
        return remote(xa.at[0, p], xa.at[k, p], xa_send.at[k, p], xa_recv.at[k, p], along[k])

    def gather_x(k, p):
        return remote(xa.at[k, p], xb.at[k, p], xb_send.at[k, p], xb_recv.at[k, p], across)

    def part_x(k, p):
        return remote(
            x_send.at[k, p], x_recv.at[k, p], px_send.at[k, p], px_recv.at[k, p], across
        )

    def part_z(k, p):
        return remote(
            z_send.at[k, p], z_recv.at[k, p], pz_send.at[k, p], pz_recv.at[k, p], along[k]
        )

    swaps = [
        remote(src, dst(1), swap_send.at[i], swap_recv.at[i], sibling)
        for i, (src, dst) in enumerate(pairs)
    ]

    order = list(range(experts))
    for p in range(pieces):
        gather_x(0, p).start()
        for k in order[1:2]:
            gather_z(k, p).start()
    for k in order[2:]:
        for p in range(pieces):
            gather_z(k, p).start()
    for swap in swaps:
        swap.start()

    smalls[2].wait()
    smalls[3].wait()
    tokens_here = ids.shape[1]
    row_at = lax.broadcasted_iota(jnp.int32, (rows, tokens_here), 0) + core * rows
    on_row = row_at == lax.broadcasted_iota(jnp.int32, (rows, tokens_here), 1)
    shares = []
    for k in range(experts):
        named = jnp.where(ids[...] == flipped(place, k, experts), weights[...], 0.0)
        line = jnp.sum(named, axis=0, keepdims=True)
        shares.append(jnp.sum(jnp.where(on_row, line, 0.0), axis=1, keepdims=True))

    def forward(k):
        for p in range(pieces):
            gather_z(k, p).wait_recv()
            gather_x(k, p).start()

    def product(k, table):
        value = None
        for p in range(pieces):
            block = jnp.concatenate([xb[k, p], xa[k, p]], axis=0)
            term = jnp.dot(block, table[part(p), :], preferred_element_type=jnp.float32)
            value = term if value is None else value + term
        return value

    def compute(k):
        for p in range(pieces):
            gather_x(k, p).wait_recv()
        if k == 0:
            loads[0].wait()
            swaps[0].wait_recv()
        gate_val = product(k, wg)
        if k == 0:
            loads[1].wait()
            swaps[1].wait_recv()
        up_val = product(k, wu)
        hidden = gated_unit(gate_val, up_val).astype(jnp.bfloat16)
        if k == 0:
            loads[2].wait()
            swaps[2].wait_recv()
        for p in range(pieces):
            result = jnp.dot(hidden, wd[:, part(p)], preferred_element_type=jnp.float32)
            x_send[k, p] = result[:rows].astype(jnp.bfloat16)
            if k:
                part_x(k, p).start()
            own_out[k, p] = result[rows:]

    def close(k):
        for p in range(pieces):
            part_x(k, p).wait_recv()
            both = own_out[k, p] + x_recv[k, p].astype(jnp.float32)
            z_send[k, p] = both.astype(jnp.bfloat16)
            part_z(k, p).start()

    for step, k in enumerate(order):
        if step + 1 < experts:
            forward(order[step + 1])
        if step >= 3:
            close(order[step - 2])
        compute(k)
    for p in range(pieces):
        part_x(0, p).start()
    for k in order[max(1, experts - 2) :]:
        close(k)

    def give(p):
        there = out_ref.at[own, part(p)]
        return remote(final.at[:, part(p)], there, last_send.at[p], last_recv.at[p], sibling)

    def keep(p):
        return pltpu.make_async_copy(
            final.at[:, part(p)], out_ref.at[own, part(p)], keep_sem.at[p]
        )

    for p in range(pieces):
        part_x(0, p).wait_recv()
        both = own_out[0, p] + x_recv[0, p].astype(jnp.float32)
        own_out[0, p] = held[:, part(p)].astype(jnp.float32) + shares[0] * both
    for p in range(pieces):
        total = own_out[0, p]
        for k in order[1:]:
            part_z(k, p).wait_recv()
            total = total + shares[k] * z_recv[k, p].astype(jnp.float32)
        final[:, part(p)] = total.astype(jnp.bfloat16)
        give(p).start()
        keep(p).start()

    for p in range(pieces):
        for k in range(experts):
            gather_x(k, p).wait_send()
            part_x(k, p).wait_send()
            if k:
                gather_z(k, p).wait_send()
                part_z(k, p).wait_send()
    for swap in swaps:
        swap.wait_send()
    for p in range(pieces):
        give(p).wait()
        keep(p).wait()


def dense_layer(tokens, gain, route_ids, route_weights, w_gate, w_up, w_down):
    experts = lax.axis_size("expert") // 2
    features = tokens.shape[1]
    rows = tokens.shape[0] // lax.axis_size("tensor")
    units = 2 * w_gate.shape[2]
    pieces = 2
    hbm = pl.BlockSpec(memory_space=pl.ANY)
    half = jnp.bfloat16
    dma = pltpu.SemaphoreType.DMA
    slots = pltpu.VMEM((experts, pieces, rows, features // pieces), half)
    ids = route_ids.T
    weights = route_weights.T
    return pl.pallas_call(
        functools.partial(dense_kernel, experts),
        out_shape=jax.ShapeDtypeStruct(tokens.shape, tokens.dtype),
        in_specs=[hbm] * 7,
        out_specs=hbm,
        scratch_shapes=[
            pltpu.VMEM((rows, features), half),
            pltpu.VMEM((features,), jnp.float32),
            pltpu.VMEM(ids.shape, jnp.int32),
            pltpu.VMEM(weights.shape, jnp.float32),
            pltpu.VMEM((features, units), half),
            pltpu.VMEM((features, units), half),
            pltpu.VMEM((units, features), half),
            slots,
            slots,
            pltpu.VMEM((experts, pieces, rows, features // pieces), jnp.float32),
            slots,
            slots,
            slots,
            slots,
            pltpu.VMEM((rows, features), half),
            dma((4,)),
            dma((3,)),
            dma((3,)),
            dma((3,)),
        ]
        + [dma((experts, pieces))] * 8
        + [dma((pieces,))] * 3,
        compiler_params=pltpu.CompilerParams(
            collective_id=0, has_side_effects=True, vmem_limit_bytes=66_000_000
        ),
    )(tokens, gain, ids, weights, w_gate, w_up, w_down)


def route_tables(chosen_ids, chosen_weights, expert_count, slot_room):
    row_count, top_count = chosen_ids.shape
    matches = (chosen_ids[:, :, None] == jnp.arange(expert_count, dtype=jnp.int32)).astype(
        jnp.float32
    )
    flat_match = matches.reshape(row_count * top_count, expert_count)
    order_range = jnp.arange(row_count * top_count, dtype=jnp.int32)
    earlier = (order_range[:, None] > order_range[None, :]).astype(jnp.float32)
    before = jnp.dot(
        earlier, flat_match, precision=lax.Precision.HIGHEST, preferred_element_type=jnp.float32
    )
    position = jnp.sum(before * flat_match, axis=1).reshape(row_count, top_count).astype(jnp.int32)
    slot_index = chosen_ids * slot_room + position
    targets = jnp.arange(expert_count * slot_room, dtype=jnp.int32)
    slot_hits = slot_index[None, :, :] == targets[:, None, None]
    send_table = jnp.sum(slot_hits.astype(jnp.float32), axis=2).astype(jnp.bfloat16)
    mix_table = jnp.sum(jnp.where(slot_hits, chosen_weights[None, :, :], 0.0), axis=2)
    return (send_table, mix_table)


def routed_layer(tokens, gain, route_ids, route_weights, w_gate, w_up, w_down):
    expert_axis = lax.axis_size("expert")
    expert_count = expert_axis // 2
    tensor_count = lax.axis_size("tensor")
    own_rows = tokens.shape[0] // tensor_count
    top_count = route_ids.shape[1]
    capacity = max(2, own_rows * top_count // expert_count)
    gate_local = w_gate[0]
    up_local = w_up[0]
    down_local = w_down[0]
    first_row = lax.axis_index("tensor") * own_rows
    own_tokens = lax.dynamic_slice_in_dim(tokens, first_row, own_rows, 0)
    own_ids = lax.dynamic_slice_in_dim(route_ids, first_row, own_rows, 0)
    own_weights = lax.dynamic_slice_in_dim(route_weights, first_row, own_rows, 0)
    resident = own_tokens.astype(jnp.float32)
    inv_rms = lax.rsqrt(jnp.mean(resident * resident, axis=1, keepdims=True) + 1e-05)
    normed = (resident * inv_rms * gain).astype(jnp.bfloat16)
    send_table, mix_table = route_tables(own_ids, own_weights, expert_count, capacity)
    packed = jnp.dot(send_table, normed, preferred_element_type=jnp.float32).astype(jnp.bfloat16)
    features = packed.shape[1]
    by_expert = packed.reshape(expert_count, 1, capacity, features)
    outgoing = jnp.broadcast_to(by_expert, (expert_count, 2, capacity, features)).reshape(
        expert_axis * capacity, features
    )
    arrived = lax.all_to_all(outgoing, "expert", split_axis=0, concat_axis=0, tiled=True)
    row_piece = lax.all_gather(arrived, "tensor", axis=0, tiled=True)
    gate_val = jnp.dot(row_piece, gate_local, preferred_element_type=jnp.float32)
    up_val = jnp.dot(row_piece, up_local, preferred_element_type=jnp.float32)
    hidden = gated_unit(gate_val, up_val).astype(jnp.bfloat16)
    partial_value = lax.psum_scatter(
        jnp.dot(hidden, down_local, preferred_element_type=jnp.float32),
        "tensor",
        scatter_dimension=0,
        tiled=True,
    )
    returned = lax.all_to_all(
        partial_value.astype(jnp.bfloat16), "expert", split_axis=0, concat_axis=0, tiled=True
    ).astype(partial_value.dtype)
    expert_out = (
        returned.reshape(expert_count, 2, capacity, features)
        .sum(axis=1)
        .reshape(expert_count * capacity, features)
    )
    weighted = jnp.dot(
        mix_table.T, expert_out, precision=lax.Precision.HIGHEST, preferred_element_type=jnp.float32
    )
    finished = (resident + weighted).astype(jnp.bfloat16)
    return lax.all_gather(finished, "tensor", axis=0, tiled=True)


def per_device(tokens, gain, route_ids, route_weights, w_gate, w_up, w_down):
    experts = lax.axis_size("expert") // 2
    dense = (
        route_ids.shape[1] == experts
        and experts & (experts - 1) == 0
        and lax.axis_size("tensor") == 2
        and w_gate.shape[0] == 1
    )
    layer = dense_layer if dense else routed_layer
    return layer(tokens, gain, route_ids, route_weights, w_gate, w_up, w_down)


def solution(mesh):
    placed = (
        P(("groups", "expert"), None),
        P(),
        P(("groups", "expert"), None),
        P(("groups", "expert"), None),
        P("expert", None, "tensor"),
        P("expert", None, "tensor"),
        P("expert", "tensor", None),
    )
    return jax.shard_map(
        per_device,
        mesh=mesh,
        in_specs=placed,
        out_specs=P(("groups", "expert"), None),
        check_vma=False,
    )
```
